256 devices in a mesh: ta: 8 (over x, core), tb: 32 (over z, y).
Axes of the slice: x: 4, y: 4, z: 8, core: 2. Of those that a mesh axis runs over, the one named last changes fastest.
Arguments:
- theta_cube: bfloat16 [256, 90, 32768], P(('ta', 'tb')), may hold values from -20 to 20, as said below
- station_permutation_map: int32 [1024], replicated, may hold values from 0 to 1023, each once
- station_bathymetry_group: int32 [32768], replicated, may hold values from 0 to 15
- baroclinic_basis: bfloat16 [16, 90, 90], replicated, may hold values from -0.625 to 0.625
Outputs:
- anomaly_coef: bfloat16 [90, 256, 32768], P(None, None, ('ta', 'tb'))
The draws below stay inside these ranges and needn't reach their ends.
Inputs may be any that keep to these rules, and one draw needn't show every extreme that they name: `theta_cube`: temperature is a level-and-column profile plus time variation.
All inputs are finite; a program needn't handle non-finite values.
Results may differ from the reference program's by a relative error of at most 0.001.
Values may be sent and summed in bfloat16 or wider, within the bound.
A program may use at most 128 MiB of HBM per device.

```python
import jax
import jax.numpy as jnp
from jax import lax

LEV = 90
MODES = 90
CLASSES = 16
TILE = 32
PROBES_PER_CHIP = 128
SNAPS = 256
COLS = 32768
GROUPS = 1024


def draw_theta_cube(key, part):
    first, second = jax.random.split(key, 2)
    profile = jax.random.uniform(first, (1, LEV, COLS), minval=-4.0, maxval=4.0)
    noise = jnp.clip(jax.random.normal(second, (SNAPS, LEV, COLS)), -6.0, 6.0)
    return (profile + noise).astype(jnp.bfloat16)


def set_ends(array, key, low, top_value):
    place = [jax.random.randint(jax.random.fold_in(key, axis), (), 0, length) for axis, length in enumerate(array.shape)]
    widest = array.shape.index(max(array.shape))
    neighbour = place[:widest] + [(place[widest] + 1) % array.shape[widest]] + place[widest + 1:]
    return array.at[tuple(place)].set(low).at[tuple(neighbour)].set(top_value)


def scatter_about(key, extent, spread, bound, kind=jnp.bfloat16):
    values = spread * jax.random.normal(key, extent, jnp.float32)
    return jnp.clip(values, min=-bound, max=bound).astype(kind)


def setup_inputs(seed: int = 0) -> dict:
    arg_keys = jax.random.split(jax.random.key(seed), 5)
    return {
        "theta_cube": draw_theta_cube(jax.random.fold_in(arg_keys[4], 71), 0),
        "station_permutation_map": jax.random.permutation(arg_keys[1], GROUPS).astype(jnp.int32),
        "station_bathymetry_group": set_ends(jax.random.randint(arg_keys[2], (COLS,), 0, CLASSES), jax.random.fold_in(arg_keys[2], 1), 0, CLASSES - 1).astype(jnp.int32),
        "baroclinic_basis": scatter_about(arg_keys[3], (CLASSES, LEV, MODES), LEV ** -0.5, 0.625),
    }


def reference(theta_cube, station_permutation_map, station_bathymetry_group, baroclinic_basis):
    offsets = jnp.arange(TILE, dtype=jnp.int32)
    source = (station_permutation_map.astype(jnp.int32)[:, None] * TILE + offsets[None, :]).reshape(-1)

    def one_block(probe_ordinal):
        probe_thermal_readings = jnp.take(theta_cube, probe_ordinal, axis=2).astype(jnp.float32)
        selected_probes = jnp.take(baroclinic_basis, jnp.take(station_bathymetry_group, probe_ordinal, axis=0), axis=0).astype(jnp.float32)
        modal_amplitude = jnp.einsum('btq,qtf->fbq', probe_thermal_readings, selected_probes)
        mean_coef = jnp.mean(modal_amplitude, axis=1, keepdims=True)
        return (modal_amplitude - mean_coef).astype(jnp.bfloat16)

    blocks = lax.map(one_block, source.reshape(-1, PROBES_PER_CHIP).astype(jnp.int32))
    return jnp.transpose(blocks, (1, 2, 0, 3)).reshape(MODES, SNAPS, COLS)
```

```python
import jax
import jax.numpy as jnp
from jax import lax
from jax.experimental import pallas as pl
from jax.experimental.pallas import tpu as pltpu
from jax.sharding import PartitionSpec as P

TILE = 32
LANES = 128
MESH = pl.DeviceIdType.MESH


def place():
    ta, tb = lax.axis_index("ta"), lax.axis_index("tb")
    return ta // 2, ta % 2, tb % 4, tb // 4


def peer(step, sign):
    x, core, y, z = place()
    turn = (step // 2) % 8
    dz = jnp.where(turn % 2 == 1, 8 - (turn + 1) // 2, turn // 2 + 1)
    dz = jnp.where(turn == 7, 0, dz)
    dy, dx = (step // 16) % 4, (step // 64) % 4
    ta = ((x + sign * dx + 4) % 4) * 2 + (core + step) % 2
    tb = ((z + sign * dz + 8) % 8) * 4 + (y + sign * dy + 4) % 4
    return ta, tb


SELF = 14


def regroup_kernel(perm, mine, group, theta, out, kind):
    levels = theta.shape[0]
    first = pl.program_id(0) * out.shape[0]
    quarter = lax.broadcasted_iota(jnp.int32, (levels, LANES), 1) // TILE

    def gathered(t, which, read):
        block = None
        for k in range(4):
            g = perm[4 * t + k]
            part = read(g // 4)
            part = pltpu.roll(part, ((k - g % 4 + 4) % 4) * TILE, 1)
            block = part if block is None else jnp.where(which == k, part, block)
        return block

    def tile_of(tile):
        return theta[:, pl.ds(pl.multiple_of(tile * LANES, LANES), LANES)]

    for i in range(out.shape[0]):
        out[i, pl.ds(0, levels), :] = gathered(first + i, quarter, tile_of)

    @pl.when(pl.program_id(0) == 0)
    def _():
        kind[...] = gathered(mine[0], quarter[:1], lambda tile: group[pl.ds(tile, 1), :])


def exchange_kernel(
    kind, basis, outbox, coef, total, inbox, modes, load_sem, send_sem, recv_sem, stage_sem
):
    levels = basis.shape[1]
    classes = basis.shape[0]
    devices = outbox.shape[0]
    ta, tb = lax.axis_index("ta"), lax.axis_index("tb")
    me = ta * 32 + tb
    here = inbox.at[me, pl.ds(0, levels)]
    load = pltpu.make_async_copy(outbox.at[me, pl.ds(0, levels)], here, load_sem)
    load.start()

    barrier = pltpu.get_barrier_semaphore()
    for d in range(1, 8):
        pl.semaphore_signal(barrier, inc=1, device_id=((ta + d) % 8, tb), device_id_type=MESH)

    def greet(d, carry):
        pl.semaphore_signal(barrier, inc=1, device_id=(ta, (tb + d) % 32), device_id_type=MESH)
        return carry

    lax.fori_loop(1, 32, greet, 0)

    def send(step):
        a, b = peer(step, 1)
        t = a * 32 + b

        @pl.when(step != SELF)
        def _():
            pltpu.make_async_remote_copy(
                src_ref=outbox.at[t, pl.ds(0, levels)],
                dst_ref=inbox.at[me, pl.ds(0, levels)],
                send_sem=send_sem,
                recv_sem=recv_sem.at[me],
                device_id=(a, b),
                device_id_type=MESH,
            ).start()

    pl.semaphore_wait(barrier, 38)
    for d in range(1, 8):
        pl.semaphore_signal(stage_sem, inc=1, device_id=((ta + d) % 8, tb), device_id_type=MESH)
    pl.semaphore_wait(stage_sem, 7)

    def send_all(step, carry):
        send(step)
        return carry

    lax.fori_loop(0, devices, send_all, 0)

    for c in range(classes):
        modes[c] = basis[c].astype(jnp.float32).T.astype(jnp.bfloat16)
    total[...] = jnp.zeros_like(total)

    def project(s):
        found = inbox[s, pl.ds(0, levels), :]
        out = jnp.zeros((levels, LANES), jnp.float32)
        for c in range(classes):
            part = jnp.dot(modes[c], found, preferred_element_type=jnp.float32)
            out = jnp.where(kind[...] == c, part, out)
        coef[:, s, :] = out
        total[...] += out

    load.wait()
    project(me)

    def receive(step, carry):
        a, b = peer(step, -1)
        s = a * 32 + b

        @pl.when(step != SELF)
        def _():
            here = inbox.at[s, pl.ds(0, levels)]
            pltpu.make_async_copy(here, here, recv_sem.at[s]).wait()
            project(s)

        return carry

    lax.fori_loop(0, devices, receive, 0)
    sent = outbox.at[pl.ds(0, devices - 1), pl.ds(0, levels)]
    pltpu.make_async_copy(sent, sent, send_sem).wait()


def centre_kernel(coef, total, out):
    snaps = out.shape[1]
    for m in range(out.shape[0]):
        mean = total[pl.program_id(0) * out.shape[0] + m][None, :] * (1.0 / snaps)
        out[m] = (coef[m, pl.ds(0, snaps), :] - mean).astype(out.dtype)


def on_device(theta_cube, station_permutation_map, station_bathymetry_group, baroclinic_basis):
    _, levels, columns = theta_cube.shape
    classes, _, mode_count = baroclinic_basis.shape
    devices = columns // LANES
    snaps = devices
    vmem = pl.BlockSpec(memory_space=pltpu.VMEM)
    me = (lax.axis_index("ta") * 32 + lax.axis_index("tb")).astype(jnp.int32).reshape(1)
    smem = pl.BlockSpec(memory_space=pltpu.SMEM)
    step = 16
    blocks, kind = pl.pallas_call(
        regroup_kernel,
        grid=(devices // step,),
        out_shape=(
            jax.ShapeDtypeStruct((devices, 96, LANES), jnp.bfloat16),
            jax.ShapeDtypeStruct((1, LANES), jnp.int32),
        ),
        in_specs=[smem, smem, vmem, vmem],
        out_specs=(pl.BlockSpec((step, 96, LANES), lambda i: (i, 0, 0)), vmem),
        name="regroup",
    )(
        station_permutation_map,
        me,
        station_bathymetry_group.reshape(columns // LANES, LANES),
        theta_cube.reshape(levels, columns),
    )
    coef, total = pl.pallas_call(
        exchange_kernel,
        out_shape=(
            jax.ShapeDtypeStruct((mode_count, snaps + 8, LANES), jnp.float32),
            jax.ShapeDtypeStruct((mode_count, LANES), jnp.float32),
        ),
        in_specs=[vmem, vmem, pl.BlockSpec(memory_space=pl.ANY)],
        out_specs=(vmem, vmem),
        scratch_shapes=[
            pltpu.VMEM((devices, 96, LANES), jnp.bfloat16),
            pltpu.VMEM((classes, mode_count, levels), jnp.bfloat16),
            pltpu.SemaphoreType.DMA,
            pltpu.SemaphoreType.DMA,
            pltpu.SemaphoreType.DMA((devices,)),
            pltpu.SemaphoreType.REGULAR,
        ],
        compiler_params=pltpu.CompilerParams(
            collective_id=0, has_side_effects=True, vmem_limit_bytes=40 * 2**20
        ),
        name="exchange",
    )(kind, baroclinic_basis, blocks)
    rows = 9
    return pl.pallas_call(
        centre_kernel,
        grid=(mode_count // rows,),
        out_shape=jax.ShapeDtypeStruct((mode_count, snaps, LANES), jnp.bfloat16),
        in_specs=[pl.BlockSpec((rows, snaps + 8, LANES), lambda i: (i, 0, 0)), vmem],
        out_specs=pl.BlockSpec((rows, snaps, LANES), lambda i: (i, 0, 0)),
        name="centre",
    )(coef, total)


def solution(mesh):
    return jax.shard_map(
        on_device,
        mesh=mesh,
        in_specs=(P(("ta", "tb"), None, None), P(), P(), P()),
        out_specs=P(None, None, ("ta", "tb")),
        check_vma=False,
    )
```

```python
import jax
import jax.numpy as jnp
from jax import lax
from jax.experimental import pallas as pl
from jax.experimental.pallas import tpu as pltpu
from jax.sharding import PartitionSpec as P

TILE = 32
LANES = 128
MESH = pl.DeviceIdType.MESH


def place():
    ta, tb = lax.axis_index("ta"), lax.axis_index("tb")
    return ta // 2, ta % 2, tb % 4, tb // 4


def peer(step, sign):
    x, core, y, z = place()
    turn, row = step % 8, step // 8
    dz = jnp.where(turn % 2 == 1, 8 - (turn + 1) // 2, turn // 2 + 1)
    dz = jnp.where(turn == 7, 0, dz)
    near = row < 4
    which = jnp.where(near, 0, (row + 3) % 7 + 1)
    dy = (jnp.where(near, row, (row - 4) // 7) + turn) % 4
    ta = ((x + sign * (which // 2) + 4) % 4) * 2 + (core + which) % 2
    tb = ((z + sign * dz + 8) % 8) * 4 + (y + sign * dy + 4) % 4
    return ta, tb


SELF = 15


def exchange_kernel(
    perm, group, basis, theta, coef, total, field, outbox, inbox, modes, load_sem, send_sem, recv_sem, stage_sem
):
    levels, columns = theta.shape
    classes = basis.shape[0]
    devices = columns // LANES
    ta, tb = lax.axis_index("ta"), lax.axis_index("tb")
    me = ta * 32 + tb

    barrier = pltpu.get_barrier_semaphore()

    def greet(d, carry):
        pl.semaphore_signal(barrier, inc=1, device_id=(ta, (tb + d) % 32), device_id_type=MESH)
        return carry

    lax.fori_loop(1, 32, greet, 0)
    for d in range(1, 8):
        pl.semaphore_signal(barrier, inc=1, device_id=((ta + d) % 8, tb), device_id_type=MESH)

    def load(i, carry):
        tile = theta.at[:, pl.ds(pl.multiple_of(i * LANES, LANES), LANES)]
        pltpu.make_async_copy(tile, field.at[i], load_sem).start()
        return carry

    lax.fori_loop(0, devices, load, 0, unroll=8)

    def gathered(t, rows, dtype, read):
        quarter = lax.broadcasted_iota(jnp.int32, (rows, LANES), 1) // TILE
        zero = jnp.zeros((rows, LANES), dtype)
        groups = [perm[4 * t + k] for k in range(4)]
        parts = [read(lax.shift_right_logical(g, 2)) for g in groups]
        block = zero
        for j in range(4):
            moved = zero
            for h in range(4):
                k = (h + j) % 4
                wanted = 4 * (groups[k] & 3) - 3 * h
                moved = jnp.where(quarter == wanted, parts[k], moved)
            block = block + (pltpu.roll(moved, j * TILE, 1) if j else moved)
        return block

    def regroup(t):
        return gathered(t, levels, jnp.bfloat16, lambda tile: field[tile])

    pltpu.make_async_copy(field, field, load_sem).wait()
    inbox[me, pl.ds(0, levels), :] = regroup(me)

    def fill(step, carry):
        a, b = peer(step, 1)
        t = a * 32 + b

        @pl.when(step != SELF)
        def _():
            outbox[t, pl.ds(0, levels), :] = regroup(t)

        return carry

    def send(step):
        a, b = peer(step, 1)
        t = a * 32 + b

        @pl.when(step != SELF)
        def _():
            pltpu.make_async_remote_copy(
                src_ref=outbox.at[t, pl.ds(0, levels)],
                dst_ref=inbox.at[me, pl.ds(0, levels)],
                send_sem=send_sem,
                recv_sem=recv_sem.at[me],
                device_id=(a, b),
                device_id_type=MESH,
            ).start()

    ahead = 4

    def fill_and_send(step, carry):
        send(step)
        fill(step + ahead, carry)
        return carry

    def send_rest(step, carry):
        send(step)
        return carry

    lax.fori_loop(0, ahead, fill, 0)
    pl.semaphore_wait(barrier, 38)
    for d in range(1, 8):
        pl.semaphore_signal(stage_sem, inc=1, device_id=((ta + d) % 8, tb), device_id_type=MESH)
    lax.fori_loop(0, 32, fill_and_send, 0)
    pl.semaphore_wait(stage_sem, 7)
    lax.fori_loop(32, devices - ahead, fill_and_send, 0)
    lax.fori_loop(devices - ahead, devices, send_rest, 0)

    kind = gathered(me, 1, jnp.int32, lambda tile: group[pl.ds(tile, 1), :])
    for c in range(classes):
        modes[c] = basis[c].astype(jnp.float32).T.astype(jnp.bfloat16)
    total[...] = jnp.zeros_like(total)

    def project(s):
        found = inbox[s, pl.ds(0, levels), :]
        out = jnp.zeros((levels, LANES), jnp.float32)
        for c in range(classes):
            part = jnp.dot(modes[c], found, preferred_element_type=jnp.float32)
            out = jnp.where(kind == c, part, out)
        coef[:, s, :] = out
        total[...] += out

    project(me)

    def receive(step, carry):
        a, b = peer(step, -1)
        s = a * 32 + b

        @pl.when(step != SELF)
        def _():
            here = inbox.at[s, pl.ds(0, levels)]
            pltpu.make_async_copy(here, here, recv_sem.at[s]).wait()
            project(s)

        return carry

    lax.fori_loop(0, devices, receive, 0)
    sent = outbox.at[pl.ds(0, devices - 1), pl.ds(0, levels)]
    pltpu.make_async_copy(sent, sent, send_sem).wait()


def centre_kernel(coef, total, out):
    rows, snaps, _ = out.shape
    first = pl.program_id(0) * rows
    for m in range(rows):
        mean = total[pl.ds(first + m, 1), :] * (1.0 / snaps)
        out[m] = (coef[first + m, pl.ds(0, snaps), :] - mean).astype(out.dtype)


def on_device(theta_cube, station_permutation_map, station_bathymetry_group, baroclinic_basis):
    _, levels, columns = theta_cube.shape
    classes, _, mode_count = baroclinic_basis.shape
    devices = columns // LANES
    snaps = devices
    vmem = pl.BlockSpec(memory_space=pltpu.VMEM)
    coef, total = pl.pallas_call(
        exchange_kernel,
        out_shape=(
            pltpu.VMEM((mode_count, snaps + 8, LANES), jnp.float32),
            pltpu.VMEM((mode_count, LANES), jnp.float32),
        ),
        in_specs=[pl.BlockSpec(memory_space=pltpu.SMEM), vmem, vmem, pl.BlockSpec(memory_space=pl.ANY)],
        out_specs=(vmem, vmem),
        scratch_shapes=[
            pltpu.VMEM((devices, levels, LANES), jnp.bfloat16),
            pltpu.VMEM((devices, 96, LANES), jnp.bfloat16),
            pltpu.VMEM((devices, 96, LANES), jnp.bfloat16),
            pltpu.VMEM((classes, mode_count, levels), jnp.bfloat16),
            pltpu.SemaphoreType.DMA,
            pltpu.SemaphoreType.DMA,
            pltpu.SemaphoreType.DMA((devices,)),
            pltpu.SemaphoreType.REGULAR,
        ],
        compiler_params=pltpu.CompilerParams(
            collective_id=0, has_side_effects=True, vmem_limit_bytes=36 * 2**20
        ),
        name="exchange",
    )(
        station_permutation_map,
        station_bathymetry_group.reshape(columns // LANES, LANES),
        baroclinic_basis,
        theta_cube.reshape(levels, columns),
    )
    rows = 9
    return pl.pallas_call(
        centre_kernel,
        grid=(mode_count // rows,),
        out_shape=jax.ShapeDtypeStruct((mode_count, snaps, LANES), jnp.bfloat16),
        in_specs=[vmem, vmem],
        out_specs=pl.BlockSpec((rows, snaps, LANES), lambda i: (i, 0, 0)),
        compiler_params=pltpu.CompilerParams(vmem_limit_bytes=8 * 2**20),
        name="centre",
    )(pltpu.with_memory_space_constraint(coef, pltpu.VMEM), pltpu.with_memory_space_constraint(total, pltpu.VMEM))


def solution(mesh):
    return jax.shard_map(
        on_device,
        mesh=mesh,
        in_specs=(P(("ta", "tb"), None, None), P(), P(), P()),
        out_specs=P(None, None, ("ta", "tb")),
        check_vma=False,
    )
```

```python
import jax
import jax.numpy as jnp
from jax import lax
from jax.experimental import pallas as pl
from jax.experimental.pallas import tpu as pltpu
from jax.sharding import PartitionSpec as P

TILE = 32
LANES = 128
MESH = pl.DeviceIdType.MESH
NEAR = 31


def at(x, core, y, z):
    return ((x + 4) % 4) * 2 + (core + 2) % 2, ((z + 8) % 8) * 4 + (y + 4) % 4


def place():
    ta, tb = lax.axis_index("ta"), lax.axis_index("tb")
    return ta // 2, ta % 2, tb % 4, tb // 4


def peer(step, sign):
    x, core, y, z = place()
    near = step < NEAR
    i = jnp.where(step >= 28, step - 27, step)
    turn, row = i % 8, i // 8
    reach = jnp.where(turn % 2 == 0, row + 1, -row - 1)
    near_z = jnp.where(step >= 28, 0, jnp.where(step >= 24, 4, reach))
    near_y = jnp.where(step >= 24, i % 4, turn // 2)
    far = step - NEAR
    turn, row = far % 8, far // 8
    far_z = jnp.where(turn % 2 == 1, -(turn + 1) // 2, turn // 2 + 1)
    far_z = jnp.where(turn == 7, 0, far_z)
    which = jnp.where(near, 0, row % 7 + 1)
    dz = jnp.where(near, near_z, far_z)
    dy = jnp.where(near, near_y, (row // 7 + turn) % 4)
    ta = ((x + sign * (which // 2) + 4) % 4) * 2 + (core + which) % 2
    tb = ((z + sign * dz + 8) % 8) * 4 + (y + sign * dy + 4) % 4
    return ta, tb


def exchange_kernel(
    perm_in, group_in, basis_in, theta, coef, total,
    perm, group, basis, field, outbox, inbox, modes,
    small_sem, load_sem, send_sem, recv_sem, stage_sem,
):
    levels, columns = theta.shape
    classes = basis_in.shape[1]
    devices = columns // LANES
    ta, tb = lax.axis_index("ta"), lax.axis_index("tb")
    me = ta * 32 + tb
    x, core, y, z = place()
    barrier = pltpu.get_barrier_semaphore()

    def tell(sem, device):
        pl.semaphore_signal(sem, inc=1, device_id=device, device_id_type=MESH)

    fetch_perm = pltpu.make_async_copy(perm_in, perm, small_sem.at[0])
    fetch_perm.start()
    for d in range(4):
        for dz in (1, -1):
            tell(barrier, at(x, core, y + d, z + dz))
    for d in range(1, 8):
        tell(barrier, ((ta + d) % 8, tb))

    def load(i, carry):
        tile = theta.at[:, pl.ds(pl.multiple_of(i * LANES, LANES), LANES)]
        pltpu.make_async_copy(tile, field.at[i], load_sem).start()
        return carry

    lax.fori_loop(0, devices, load, 0, unroll=8)
    fetch_group = pltpu.make_async_copy(group_in, group, small_sem.at[1])
    fetch_basis = pltpu.make_async_copy(basis_in, basis, small_sem.at[2])
    fetch_group.start()
    fetch_basis.start()

    def gathered(t, rows, dtype, read):
        quarter = lax.broadcasted_iota(jnp.int32, (rows, LANES), 1) // TILE
        zero = jnp.zeros((rows, LANES), dtype)
        groups = [perm[4 * t + k] for k in range(4)]
        parts = [read(lax.shift_right_logical(g, 2)) for g in groups]
        block = None
        for j in range(4):
            moved = zero
            for h in range(4):
                k = (h + j) % 4
                wanted = 4 * (groups[k] & 3) - 3 * h
                moved = jnp.where(quarter == wanted, parts[k], moved)
            moved = pltpu.roll(moved, j * TILE, 1) if j else moved
            block = moved if block is None else block + moved
        return block

    def regroup(t):
        return gathered(t, levels, jnp.bfloat16, lambda tile: field[tile])

    def fill(step, carry):
        a, b = peer(step, 1)
        t = a * 32 + b
        outbox[t, pl.ds(0, levels), :] = regroup(t)
        return carry

    def send(step, carry):
        a, b = peer(step, 1)
        t = a * 32 + b
        pltpu.make_async_remote_copy(
            src_ref=outbox.at[t, pl.ds(0, levels)],
            dst_ref=inbox.at[me, pl.ds(0, levels)],
            send_sem=send_sem,
            recv_sem=recv_sem.at[me],
            device_id=(a, b),
            device_id_type=MESH,
        ).start()
        return carry

    ahead = 4

    def send_and_fill(step, carry):
        send(step, carry)
        fill(step + ahead, carry)
        return carry

    fetch_perm.wait()
    pltpu.make_async_copy(field, field, load_sem).wait()
    lax.fori_loop(0, ahead, fill, 0)
    pl.semaphore_wait(barrier, 15)
    for dz in (1, -1):
        tell(stage_sem.at[0], at(x, core, y, z + dz))
    lax.fori_loop(0, 8, send_and_fill, 0)
    pl.semaphore_wait(stage_sem.at[0], 2)
    for dz in (2, -2):
        tell(stage_sem.at[1], at(x, core, y, z + dz))
    lax.fori_loop(8, 16, send_and_fill, 0)
    pl.semaphore_wait(stage_sem.at[1], 2)
    for d in range(1, 8):
        tell(stage_sem.at[2], ((ta + d) % 8, tb))
    lax.fori_loop(16, NEAR, send_and_fill, 0)
    pl.semaphore_wait(stage_sem.at[2], 7)
    lax.fori_loop(NEAR, devices - 1 - ahead, send_and_fill, 0)
    lax.fori_loop(devices - 1 - ahead, devices - 1, send, 0)

    inbox[me, pl.ds(0, levels), :] = regroup(me)
    fetch_group.wait()
    kind = gathered(me, 1, jnp.int32, lambda tile: group[pl.ds(tile, 1), :])
    kind = jnp.concatenate([kind, kind], axis=1)
    fetch_basis.wait()
    for c in range(classes):
        modes[c] = basis[:, c, :].astype(jnp.float32).T.astype(jnp.bfloat16)
    total[...] = jnp.zeros_like(total)

    def project(first, second):
        found = jnp.concatenate([inbox[first, pl.ds(0, levels), :], inbox[second, pl.ds(0, levels), :]], axis=1)
        out = jnp.zeros((total.shape[0], 2 * LANES), jnp.float32)
        for c in range(classes):
            part = jnp.dot(modes[c], found, preferred_element_type=jnp.float32)
            out = jnp.where(kind == c, part, out)
        coef[:, first, :] = out[:, :LANES]
        coef[:, second, :] = out[:, LANES:]
        total[...] += out[:, :LANES] + out[:, LANES:]

    def arrived(step):
        a, b = peer(step, -1)
        s = a * 32 + b
        here = inbox.at[s, pl.ds(0, levels)]
        pltpu.make_async_copy(here, here, recv_sem.at[s]).wait()
        return s

    project(me, arrived(0))

    def receive(i, carry):
        first = arrived(2 * i + 1)
        project(first, arrived(2 * i + 2))
        return carry

    lax.fori_loop(0, (devices - 2) // 2, receive, 0)
    sent = outbox.at[pl.ds(0, devices - 1), pl.ds(0, levels)]
    pltpu.make_async_copy(sent, sent, send_sem).wait()


def centre_kernel(coef, total, out):
    rows, snaps, _ = out.shape
    first = pl.program_id(0) * rows
    for m in range(rows):
        mean = total[pl.ds(first + m, 1), :] * (1.0 / snaps)
        out[m] = (coef[first + m, pl.ds(0, snaps), :] - mean).astype(out.dtype)


def on_device(theta_cube, station_permutation_map, station_bathymetry_group, baroclinic_basis):
    _, levels, columns = theta_cube.shape
    classes, _, mode_count = baroclinic_basis.shape
    devices = columns // LANES
    snaps = devices
    vmem = pl.BlockSpec(memory_space=pltpu.VMEM)
    hbm = pl.BlockSpec(memory_space=pl.ANY)
    coef, total = pl.pallas_call(
        exchange_kernel,
        out_shape=(
            pltpu.VMEM((mode_count, snaps + 8, LANES), jnp.float32),
            pltpu.VMEM((mode_count, LANES), jnp.float32),
        ),
        in_specs=[hbm] * 4,
        out_specs=(vmem, vmem),
        scratch_shapes=[
            pltpu.SMEM((columns // TILE,), jnp.int32),
            pltpu.VMEM((devices, LANES), jnp.int32),
            pltpu.VMEM((levels, classes, mode_count), jnp.bfloat16),
            pltpu.VMEM((devices, levels, LANES), jnp.bfloat16),
            pltpu.VMEM((devices, 96, LANES), jnp.bfloat16),
            pltpu.VMEM((devices, 96, LANES), jnp.bfloat16),
            pltpu.VMEM((classes, mode_count, levels), jnp.bfloat16),
            pltpu.SemaphoreType.DMA((3,)),
            pltpu.SemaphoreType.DMA,
            pltpu.SemaphoreType.DMA,
            pltpu.SemaphoreType.DMA((devices,)),
            pltpu.SemaphoreType.REGULAR((3,)),
        ],
        compiler_params=pltpu.CompilerParams(
            collective_id=0, has_side_effects=True, vmem_limit_bytes=36 * 2**20
        ),
        name="exchange",
    )(*(pltpu.with_memory_space_constraint(a, pltpu.HBM) for a in (
        station_permutation_map,
        station_bathymetry_group.reshape(columns // LANES, LANES),
        baroclinic_basis.transpose(1, 0, 2),
        theta_cube.reshape(levels, columns),
    )))
    rows = 9
    return pl.pallas_call(
        centre_kernel,
        grid=(mode_count // rows,),
        out_shape=jax.ShapeDtypeStruct((mode_count, snaps, LANES), jnp.bfloat16),
        in_specs=[vmem, vmem],
        out_specs=pl.BlockSpec((rows, snaps, LANES), lambda i: (i, 0, 0)),
        compiler_params=pltpu.CompilerParams(vmem_limit_bytes=8 * 2**20),
        name="centre",
    )(pltpu.with_memory_space_constraint(coef, pltpu.VMEM), pltpu.with_memory_space_constraint(total, pltpu.VMEM))


def solution(mesh):
    return jax.shard_map(
        on_device,
        mesh=mesh,
        in_specs=(P(("ta", "tb"), None, None), P(), P(), P()),
        out_specs=P(None, None, ("ta", "tb")),
        check_vma=False,
    )
```

```python
import jax
import jax.numpy as jnp
from jax import lax
from jax.experimental import pallas as pl
from jax.experimental.pallas import tpu as pltpu
from jax.sharding import PartitionSpec as P

TILE = 32
LANES = 128
MESH = pl.DeviceIdType.MESH
NEAR = 31


def at(x, core, y, z):
    return ((x + 4) % 4) * 2 + (core + 2) % 2, ((z + 8) % 8) * 4 + (y + 4) % 4


def place():
    ta, tb = lax.axis_index("ta"), lax.axis_index("tb")
    return ta // 2, ta % 2, tb % 4, tb // 4


def peer(step, sign):
    x, core, y, z = place()
    near = step < NEAR
    i = jnp.where(step >= 28, step - 27, step)
    turn, row = i % 8, i // 8
    reach = jnp.where(turn % 2 == 0, row + 1, -row - 1)
    near_z = jnp.where(step >= 28, 0, jnp.where(step >= 24, 4, reach))
    near_y = jnp.where(step >= 24, i % 4, turn // 2)
    far = step - NEAR
    turn, row = far % 8, far // 8
    far_z = jnp.where(turn % 2 == 1, -(turn + 1) // 2, turn // 2 + 1)
    far_z = jnp.where(turn == 7, 0, far_z)
    which = jnp.where(near, 0, row % 7 + 1)
    dz = jnp.where(near, near_z, far_z)
    dy = jnp.where(near, near_y, (row // 7 + turn) % 4)
    ta = ((x + sign * (which // 2) + 4) % 4) * 2 + (core + which) % 2
    tb = ((z + sign * dz + 8) % 8) * 4 + (y + sign * dy + 4) % 4
    return ta, tb


def exchange_kernel(
    perm_in, group_in, basis_in, theta, coef, total,
    perm, group, basis, field, outbox, inbox, modes,
    small_sem, load_sem, send_sem, recv_sem, stage_sem,
):
    levels, columns = theta.shape
    classes = basis_in.shape[1]
    devices = columns // LANES
    ta, tb = lax.axis_index("ta"), lax.axis_index("tb")
    me = ta * 32 + tb
    x, core, y, z = place()
    barrier = pltpu.get_barrier_semaphore()

    def tell(sem, device):
        pl.semaphore_signal(sem, inc=1, device_id=device, device_id_type=MESH)

    fetch_perm = pltpu.make_async_copy(perm_in, perm, small_sem.at[0])
    load = pltpu.make_async_copy(theta, field, load_sem)
    fetch_perm.start()
    load.start()
    for d in range(4):
        for dz in (1, -1):
            tell(barrier, at(x, core, y + d, z + dz))
    for d in range(1, 8):
        tell(barrier, ((ta + d) % 8, tb))

    fetch_group = pltpu.make_async_copy(group_in, group, small_sem.at[1])
    fetch_basis = pltpu.make_async_copy(basis_in, basis, small_sem.at[2])
    fetch_group.start()
    fetch_basis.start()

    def gathered(t, rows, dtype, read):
        quarter = lax.broadcasted_iota(jnp.int32, (rows, LANES), 1) // TILE
        zero = jnp.zeros((rows, LANES), dtype)
        groups = [perm[4 * t + k] for k in range(4)]
        parts = [read(lax.shift_right_logical(g, 2)) for g in groups]
        block = None
        for j in range(4):
            moved = zero
            for h in range(4):
                k = (h + j) % 4
                wanted = 4 * (groups[k] & 3) - 3 * h
                moved = jnp.where(quarter == wanted, parts[k], moved)
            moved = pltpu.roll(moved, j * TILE, 1) if j else moved
            block = moved if block is None else block + moved
        return block

    def regroup(t):
        return gathered(t, levels, jnp.bfloat16, lambda tile: field[:, pl.ds(tile * LANES, LANES)])

    def fill(step, carry):
        a, b = peer(step, 1)
        t = a * 32 + b
        outbox[t, pl.ds(0, levels), :] = regroup(t)
        return carry

    def send(step, carry):
        a, b = peer(step, 1)
        t = a * 32 + b
        pltpu.make_async_remote_copy(
            src_ref=outbox.at[t, pl.ds(0, levels)],
            dst_ref=inbox.at[me, pl.ds(0, levels)],
            send_sem=send_sem,
            recv_sem=recv_sem.at[me],
            device_id=(a, b),
            device_id_type=MESH,
        ).start()
        return carry

    ahead = 2

    def send_and_fill(step, carry):
        send(step, carry)
        fill(step + ahead, carry)
        return carry

    fetch_perm.wait()
    load.wait()
    lax.fori_loop(0, ahead, fill, 0)
    pl.semaphore_wait(barrier, 15)
    for dz in (1, -1):
        tell(stage_sem.at[0], at(x, core, y, z + dz))
    lax.fori_loop(0, 8, send_and_fill, 0)
    pl.semaphore_wait(stage_sem.at[0], 2)
    for dz in (2, -2):
        tell(stage_sem.at[1], at(x, core, y, z + dz))
    lax.fori_loop(8, 16, send_and_fill, 0)
    pl.semaphore_wait(stage_sem.at[1], 2)
    for d in range(1, 8):
        tell(stage_sem.at[2], ((ta + d) % 8, tb))
    lax.fori_loop(16, NEAR, send_and_fill, 0)
    pl.semaphore_wait(stage_sem.at[2], 7)
    lax.fori_loop(NEAR, devices - 1 - ahead, send_and_fill, 0)
    lax.fori_loop(devices - 1 - ahead, devices - 1, send, 0)

    inbox[me, pl.ds(0, levels), :] = regroup(me)
    fetch_group.wait()
    kind = gathered(me, 1, jnp.int32, lambda tile: group[pl.ds(tile, 1), :])
    kind = jnp.concatenate([kind, kind], axis=1)
    fetch_basis.wait()
    for c in range(classes):
        modes[c] = basis[:, c, :].astype(jnp.float32).T.astype(jnp.bfloat16)
    total[...] = jnp.zeros_like(total)

    def project(first, second):
        found = jnp.concatenate([inbox[first, pl.ds(0, levels), :], inbox[second, pl.ds(0, levels), :]], axis=1)
        out = jnp.zeros((total.shape[0], 2 * LANES), jnp.float32)
        for c in range(classes):
            part = jnp.dot(modes[c], found, preferred_element_type=jnp.float32)
            out = jnp.where(kind == c, part, out)
        coef[:, first, :] = out[:, :LANES]
        coef[:, second, :] = out[:, LANES:]
        total[...] += out[:, :LANES] + out[:, LANES:]

    def arrived(step):
        a, b = peer(step, -1)
        s = a * 32 + b
        here = inbox.at[s, pl.ds(0, levels)]
        pltpu.make_async_copy(here, here, recv_sem.at[s]).wait()
        return s

    project(me, arrived(0))

    def receive(i, carry):
        first = arrived(2 * i + 1)
        project(first, arrived(2 * i + 2))
        return carry

    lax.fori_loop(0, (devices - 2) // 2, receive, 0)
    sent = outbox.at[pl.ds(0, devices - 1), pl.ds(0, levels)]
    pltpu.make_async_copy(sent, sent, send_sem).wait()


def centre_kernel(coef, total, out, rounded, sem):
    modes, snaps, _ = out.shape
    rows = 2

    def part(i, carry):
        for m in range(rows):
            mean = total[pl.ds(i * rows + m, 1), :] * (1.0 / snaps)
            rounded[i * rows + m] = (coef[i * rows + m, pl.ds(0, snaps), :] - mean).astype(out.dtype)
        here = pl.ds(i * rows, rows)
        pltpu.make_async_copy(rounded.at[here], out.at[here], sem).start()
        return carry

    lax.fori_loop(0, modes // rows, part, 0)
    pltpu.make_async_copy(rounded, out, sem).wait()


def on_device(theta_cube, station_permutation_map, station_bathymetry_group, baroclinic_basis):
    _, levels, columns = theta_cube.shape
    classes, _, mode_count = baroclinic_basis.shape
    devices = columns // LANES
    snaps = devices
    vmem = pl.BlockSpec(memory_space=pltpu.VMEM)
    hbm = pl.BlockSpec(memory_space=pl.ANY)
    coef, total = pl.pallas_call(
        exchange_kernel,
        out_shape=(
            pltpu.VMEM((mode_count, snaps + 8, LANES), jnp.float32),
            pltpu.VMEM((mode_count, LANES), jnp.float32),
        ),
        in_specs=[hbm] * 4,
        out_specs=(vmem, vmem),
        scratch_shapes=[
            pltpu.SMEM((columns // TILE,), jnp.int32),
            pltpu.VMEM((devices, LANES), jnp.int32),
            pltpu.VMEM((levels, classes, mode_count), jnp.bfloat16),
            pltpu.VMEM((levels, columns), jnp.bfloat16),
            pltpu.VMEM((devices, 96, LANES), jnp.bfloat16),
            pltpu.VMEM((devices, 96, LANES), jnp.bfloat16),
            pltpu.VMEM((classes, mode_count, levels), jnp.bfloat16),
            pltpu.SemaphoreType.DMA((3,)),
            pltpu.SemaphoreType.DMA,
            pltpu.SemaphoreType.DMA,
            pltpu.SemaphoreType.DMA((devices,)),
            pltpu.SemaphoreType.REGULAR((3,)),
        ],
        compiler_params=pltpu.CompilerParams(
            collective_id=0, has_side_effects=True, vmem_limit_bytes=36 * 2**20
        ),
        name="exchange",
    )(*(pltpu.with_memory_space_constraint(a, pltpu.HBM) for a in (
        station_permutation_map,
        station_bathymetry_group.reshape(columns // LANES, LANES),
        baroclinic_basis.transpose(1, 0, 2),
        theta_cube.reshape(levels, columns),
    )))
    return pl.pallas_call(
        centre_kernel,
        out_shape=jax.ShapeDtypeStruct((mode_count, snaps, LANES), jnp.bfloat16),
        in_specs=[vmem, vmem],
        out_specs=hbm,
        scratch_shapes=[pltpu.VMEM((mode_count, snaps, LANES), jnp.bfloat16), pltpu.SemaphoreType.DMA],
        compiler_params=pltpu.CompilerParams(vmem_limit_bytes=12 * 2**20),
        name="centre",
    )(pltpu.with_memory_space_constraint(coef, pltpu.VMEM), pltpu.with_memory_space_constraint(total, pltpu.VMEM))


def solution(mesh):
    return jax.shard_map(
        on_device,
        mesh=mesh,
        in_specs=(P(("ta", "tb"), None, None), P(), P(), P()),
        out_specs=P(None, None, ("ta", "tb")),
        check_vma=False,
    )
```

```python
import jax
import jax.numpy as jnp
from jax import lax
from jax.experimental import pallas as pl
from jax.experimental.pallas import tpu as pltpu
from jax.sharding import PartitionSpec as P

TILE = 32
LANES = 128
MESH = pl.DeviceIdType.MESH
NEAR = 31


def at(x, core, y, z):
    return ((x + 4) % 4) * 2 + (core + 2) % 2, ((z + 8) % 8) * 4 + (y + 4) % 4


def place():
    ta, tb = lax.axis_index("ta"), lax.axis_index("tb")
    return ta // 2, ta % 2, tb % 4, tb // 4


def peer(step, sign):
    x, core, y, z = place()
    near = step < NEAR
    i = jnp.where(step >= 28, step - 27, step)
    turn, row = i % 8, i // 8
    reach = jnp.where(turn % 2 == 0, row + 1, -row - 1)
    near_z = jnp.where(step >= 28, 0, jnp.where(step >= 24, 4, reach))
    near_y = jnp.where(step >= 24, i % 4, turn // 2)
    far = step - NEAR
    late, k, m = far >= 184, far - 184, far % 46
    full = m < 16
    pick = jnp.where(late, (k % 10 // 2 + 1) % 5, (m - 16) // 6)
    pick = pick + jnp.where(pick >= 3, 3, 1)
    which = jnp.where(near, 0, jnp.where(late, pick, jnp.where(full, 4 + m // 8, pick)))
    turn = jnp.where(late, k % 2, jnp.where(full, m % 8, 2 + (m - 16) % 6))
    far_z = jnp.where(turn % 2 == 1, -((turn + 1) // 2), turn // 2 + 1)
    far_z = jnp.where(turn == 7, 0, far_z)
    late_y = jnp.where(k // 10 == 3, 0, jnp.where(k // 10 == 2, 3, 2 - k // 10))
    dz = jnp.where(near, near_z, far_z)
    dy = jnp.where(near, near_y, jnp.where(late, late_y, (far // 46 + turn) % 4))
    ta = ((x + sign * (which // 2) + 4) % 4) * 2 + (core + which) % 2
    tb = ((z + sign * dz + 8) % 8) * 4 + (y + sign * dy + 4) % 4
    return ta, tb


def exchange_kernel(
    perm_in, group_in, basis_in, theta, coef, total,
    perm, group, basis, field, outbox, inbox, modes,
    small_sem, load_sem, send_sem, recv_sem, stage_sem,
):
    levels, columns = theta.shape
    classes = basis_in.shape[1]
    devices = columns // LANES
    ta, tb = lax.axis_index("ta"), lax.axis_index("tb")
    me = ta * 32 + tb
    x, core, y, z = place()
    barrier = pltpu.get_barrier_semaphore()

    def tell(sem, device):
        pl.semaphore_signal(sem, inc=1, device_id=device, device_id_type=MESH)

    fetch_perm = pltpu.make_async_copy(perm_in, perm, small_sem.at[0])
    load = pltpu.make_async_copy(theta, field, load_sem)
    fetch_perm.start()
    load.start()
    for d in range(4):
        for dz in (1, -1):
            tell(barrier, at(x, core, y + d, z + dz))
    for d in range(1, 8):
        tell(barrier, ((ta + d) % 8, tb))

    fetch_group = pltpu.make_async_copy(group_in, group, small_sem.at[1])
    fetch_basis = pltpu.make_async_copy(basis_in, basis, small_sem.at[2])
    fetch_group.start()
    fetch_basis.start()

    def gathered(t, rows, dtype, read):
        quarter = lax.broadcasted_iota(jnp.int32, (rows, LANES), 1) // TILE
        zero = jnp.zeros((rows, LANES), dtype)
        groups = [perm[4 * t + k] for k in range(4)]
        parts = [read(lax.shift_right_logical(g, 2)) for g in groups]
        block = None
        for j in range(4):
            moved = zero
            for h in range(4):
                k = (h + j) % 4
                wanted = 4 * (groups[k] & 3) - 3 * h
                moved = jnp.where(quarter == wanted, parts[k], moved)
            moved = pltpu.roll(moved, j * TILE, 1) if j else moved
            block = moved if block is None else block + moved
        return block

    def regroup(t):
        return gathered(t, levels, jnp.bfloat16, lambda tile: field[:, pl.ds(tile * LANES, LANES)])

    def fill(step, carry):
        a, b = peer(step, 1)
        t = a * 32 + b
        outbox[t, pl.ds(0, levels), :] = regroup(t)
        return carry

    def send(step, carry):
        a, b = peer(step, 1)
        t = a * 32 + b
        pltpu.make_async_remote_copy(
            src_ref=outbox.at[t, pl.ds(0, levels)],
            dst_ref=inbox.at[me, pl.ds(0, levels)],
            send_sem=send_sem,
            recv_sem=recv_sem.at[me],
            device_id=(a, b),
            device_id_type=MESH,
        ).start()
        return carry

    ahead = 2

    def send_and_fill(step, carry):
        send(step, carry)
        fill(step + ahead, carry)
        return carry

    fetch_perm.wait()
    load.wait()
    lax.fori_loop(0, ahead, fill, 0)
    pl.semaphore_wait(barrier, 15)
    for dz in (1, -1):
        tell(stage_sem.at[0], at(x, core, y, z + dz))
    lax.fori_loop(0, 8, send_and_fill, 0)
    pl.semaphore_wait(stage_sem.at[0], 2)
    for dz in (2, -2):
        tell(stage_sem.at[1], at(x, core, y, z + dz))
    lax.fori_loop(8, 16, send_and_fill, 0)
    pl.semaphore_wait(stage_sem.at[1], 2)
    for d in range(1, 8):
        tell(stage_sem.at[2], ((ta + d) % 8, tb))
    lax.fori_loop(16, NEAR, send_and_fill, 0)
    pl.semaphore_wait(stage_sem.at[2], 7)
    lax.fori_loop(NEAR, devices - 1 - ahead, send_and_fill, 0)
    lax.fori_loop(devices - 1 - ahead, devices - 1, send, 0)

    inbox[me, pl.ds(0, levels), :] = regroup(me)
    fetch_group.wait()
    kind = gathered(me, 1, jnp.int32, lambda tile: group[pl.ds(tile, 1), :])
    kind = jnp.concatenate([kind, kind], axis=1)
    fetch_basis.wait()
    for c in range(classes):
        modes[c] = basis[:, c, :].astype(jnp.float32).T.astype(jnp.bfloat16)
    total[...] = jnp.zeros_like(total)

    def project(first, second):
        found = jnp.concatenate([inbox[first, pl.ds(0, levels), :], inbox[second, pl.ds(0, levels), :]], axis=1)
        out = jnp.zeros((total.shape[0], 2 * LANES), jnp.float32)
        for c in range(classes):
            part = jnp.dot(modes[c], found, preferred_element_type=jnp.float32)
            out = jnp.where(kind == c, part, out)
        coef[:, first, :] = out[:, :LANES]
        coef[:, second, :] = out[:, LANES:]
        total[...] += out[:, :LANES] + out[:, LANES:]

    def arrived(step):
        a, b = peer(step, -1)
        s = a * 32 + b
        here = inbox.at[s, pl.ds(0, levels)]
        pltpu.make_async_copy(here, here, recv_sem.at[s]).wait()
        return s

    project(me, arrived(0))

    def receive(i, carry):
        first = arrived(2 * i + 1)
        project(first, arrived(2 * i + 2))
        return carry

    lax.fori_loop(0, (devices - 2) // 2, receive, 0)
    sent = outbox.at[pl.ds(0, devices - 1), pl.ds(0, levels)]
    pltpu.make_async_copy(sent, sent, send_sem).wait()


def centre_kernel(coef, total, out, rounded, sem):
    modes, snaps, _ = out.shape
    rows = 2

    def part(i, carry):
        for m in range(rows):
            mean = total[pl.ds(i * rows + m, 1), :] * (1.0 / snaps)
            rounded[i * rows + m] = (coef[i * rows + m, pl.ds(0, snaps), :] - mean).astype(out.dtype)
        here = pl.ds(i * rows, rows)
        pltpu.make_async_copy(rounded.at[here], out.at[here], sem).start()
        return carry

    lax.fori_loop(0, modes // rows, part, 0)
    pltpu.make_async_copy(rounded, out, sem).wait()


def on_device(theta_cube, station_permutation_map, station_bathymetry_group, baroclinic_basis):
    _, levels, columns = theta_cube.shape
    classes, _, mode_count = baroclinic_basis.shape
    devices = columns // LANES
    snaps = devices
    vmem = pl.BlockSpec(memory_space=pltpu.VMEM)
    hbm = pl.BlockSpec(memory_space=pl.ANY)
    coef, total = pl.pallas_call(
        exchange_kernel,
        out_shape=(
            pltpu.VMEM((mode_count, snaps + 8, LANES), jnp.float32),
            pltpu.VMEM((mode_count, LANES), jnp.float32),
        ),
        in_specs=[hbm] * 4,
        out_specs=(vmem, vmem),
        scratch_shapes=[
            pltpu.SMEM((columns // TILE,), jnp.int32),
            pltpu.VMEM((devices, LANES), jnp.int32),
            pltpu.VMEM((levels, classes, mode_count), jnp.bfloat16),
            pltpu.VMEM((levels, columns), jnp.bfloat16),
            pltpu.VMEM((devices, 96, LANES), jnp.bfloat16),
            pltpu.VMEM((devices, 96, LANES), jnp.bfloat16),
            pltpu.VMEM((classes, mode_count, levels), jnp.bfloat16),
            pltpu.SemaphoreType.DMA((3,)),
            pltpu.SemaphoreType.DMA,
            pltpu.SemaphoreType.DMA,
            pltpu.SemaphoreType.DMA((devices,)),
            pltpu.SemaphoreType.REGULAR((3,)),
        ],
        compiler_params=pltpu.CompilerParams(
            collective_id=0, has_side_effects=True, vmem_limit_bytes=36 * 2**20
        ),
        name="exchange",
    )(*(pltpu.with_memory_space_constraint(a, pltpu.HBM) for a in (
        station_permutation_map,
        station_bathymetry_group.reshape(columns // LANES, LANES),
        baroclinic_basis.transpose(1, 0, 2),
        theta_cube.reshape(levels, columns),
    )))
    return pl.pallas_call(
        centre_kernel,
        out_shape=jax.ShapeDtypeStruct((mode_count, snaps, LANES), jnp.bfloat16),
        in_specs=[vmem, vmem],
        out_specs=hbm,
        scratch_shapes=[pltpu.VMEM((mode_count, snaps, LANES), jnp.bfloat16), pltpu.SemaphoreType.DMA],
        compiler_params=pltpu.CompilerParams(vmem_limit_bytes=12 * 2**20),
        name="centre",
    )(pltpu.with_memory_space_constraint(coef, pltpu.VMEM), pltpu.with_memory_space_constraint(total, pltpu.VMEM))


def solution(mesh):
    return jax.shard_map(
        on_device,
        mesh=mesh,
        in_specs=(P(("ta", "tb"), None, None), P(), P(), P()),
        out_specs=P(None, None, ("ta", "tb")),
        check_vma=False,
    )
```
